32 devices in a mesh: ep: 4 (over y, x), fsdp: 8 (over z, core).
Axes of the slice: x: 2, y: 2, z: 4, core: 2. Of those that a mesh axis runs over, the one named last changes fastest.
Arguments:
- train_gate: float32 [128, 2048, 768], P('ep', 'fsdp'), may hold values from -0.1875 to 0.1875
- other_gate: bfloat16 [128, 2048, 768], P('ep', 'fsdp'), may hold values from -0.0625 to 0.0625
- train_up: float32 [128, 2048, 768], P('ep', 'fsdp'), may hold values from -0.1875 to 0.1875
- other_up: bfloat16 [128, 2048, 768], P('ep', 'fsdp'), may hold values from -0.0625 to 0.0625
- router_weight: float32 [2048, 128], P('fsdp', 'ep'), may hold values from -0.125 to 0.125
- router_gain: float32 [2048], P('fsdp'), may hold values from 0.25 to 1.75
Outputs:
- ready_gate: bfloat16 [128, 2048, 768], P(('ep', 'fsdp'))
- ready_up: bfloat16 [128, 2048, 768], P(('ep', 'fsdp'))
- scale_gate: float32 [128, 768], P(('ep', 'fsdp'))
- scale_up: float32 [128, 768], P(('ep', 'fsdp'))
- serve_router: bfloat16 [2048, 128], replicated
The draws below stay inside these ranges and needn't reach their ends.
All inputs are finite; a program needn't handle non-finite values. Where the reference program divides by a largest or mean magnitude, that divisor is 1e-20 or more.
Results may differ from the reference program's by a relative error of at most 0.013.
Values may be sent and summed in bfloat16 or wider, within the bound.
A program may use at most 192 MiB of HBM per device.

```python
import jax
import jax.numpy as jnp

EXPERTS = 128
D_MODEL = 2048
D_EXPERT = 768


def raised(drawn, key, source, target, shards_of, factor):
    def block_of(dim):
        return (jnp.arange(drawn.shape[dim]) // (drawn.shape[dim] // shards_of)).reshape((-1,) + (1,) * (drawn.ndim - 1 - dim))

    first = jax.random.permutation(key, shards_of)[block_of(target)]
    second = (block_of(target) + shards_of // 2) % shards_of
    return jnp.where((block_of(source) == first) | (block_of(source) == second), factor * drawn, drawn)


def steps_of(own_key, shape, shards, smallest, top_value):
    gain, own = 1.0, jax.random.fold_in(own_key, 6)
    for position, parts in shards:
        steps = jnp.exp(jax.random.uniform(jax.random.fold_in(own, position), (parts,), jnp.float32, smallest / len(shards), top_value / len(shards)))
        gain = gain * jnp.repeat(steps, shape[position] // parts).reshape([-1 if axis == position else 1 for axis in range(len(shape))])
    return gain


def gaussian(rng, shape, scale, most, pieces=(), kind=jnp.bfloat16):
    loudness = steps_of(rng, shape, pieces, -0.22, 0.18) if pieces else 1.0
    values = jax.random.normal(rng, shape, jnp.float32) * scale * loudness
    return jnp.minimum(jnp.maximum(values, -most), most).astype(kind)


def noise_with(rng, shape, width, most, shards, heavy, held_as=jnp.bfloat16):
    array = width * jax.random.normal(rng, shape, jnp.float32)
    if shards:
        array = array * steps_of(rng, shape, shards, -0.22, 0.18)
    return jnp.clip(raised(array, jax.random.fold_in(rng, 3), *heavy), -most, most).astype(held_as)


def setup_inputs(seed: int = 0) -> dict:
    arg_keys = jax.random.split(jax.random.key(seed), 7)
    return {
        "train_gate": noise_with(arg_keys[0], (EXPERTS, D_MODEL, D_EXPERT), D_MODEL ** -0.5, 0.1875, ((0, 4), (1, 8)), (1, 2, 8, 2.0), jnp.float32),
        "other_gate": gaussian(arg_keys[1], (EXPERTS, D_MODEL, D_EXPERT), (D_MODEL * 4) ** -0.5, 0.0625, ((0, 4), (1, 8))),
        "train_up": noise_with(arg_keys[2], (EXPERTS, D_MODEL, D_EXPERT), D_MODEL ** -0.5, 0.1875, ((0, 4), (1, 8)), (1, 2, 8, 2.0), jnp.float32),
        "other_up": gaussian(arg_keys[3], (EXPERTS, D_MODEL, D_EXPERT), (D_MODEL * 4) ** -0.5, 0.0625, ((0, 4), (1, 8))),
        "router_weight": gaussian(arg_keys[4], (D_MODEL, EXPERTS), D_MODEL ** -0.5, 0.125, ((0, 8), (1, 4)), jnp.float32),
        "router_gain": jnp.clip(1.0 + 0.15 * jax.random.normal(arg_keys[5], (D_MODEL,), jnp.float32), 0.25, 1.75),
    }


def reference(train_gate, other_gate, train_up, other_up, router_weight, router_gain):
    latest_gate = train_gate + other_gate.astype(jnp.float32)
    latest_up = train_up + other_up.astype(jnp.float32)
    scale_gate = jnp.sum(jnp.abs(latest_gate), axis=1) / D_MODEL
    ready_gate = (latest_gate / jnp.expand_dims(scale_gate, 1)).astype(jnp.bfloat16)
    scale_up = jnp.sum(jnp.abs(latest_up), axis=1) / D_MODEL
    ready_up = (latest_up / jnp.expand_dims(scale_up, 1)).astype(jnp.bfloat16)
    serve_router = (router_weight * router_gain[:, None]).astype(jnp.bfloat16)
    return ready_gate, ready_up, scale_gate, scale_up, serve_router
```

```python
import functools

import jax
import jax.numpy as jnp
from jax import lax
from jax.experimental import pallas as pl
from jax.experimental.pallas import tpu as pltpu
from jax.sharding import PartitionSpec as P

MESH = pl.DeviceIdType.MESH
SLOTS = 4
ROWS = 32


def exchange(
    n,
    groups,
    train_gate,
    other_gate,
    train_up,
    other_up,
    router,
    out_gate,
    out_up,
    out_router,
    wide,
    narrow,
    send,
    wide_sem,
    narrow_sem,
    send_sem,
    gate_sem,
    up_sem,
    row_send,
    row_recv,
    col_send,
    col_recv,
):
    me = lax.axis_index("fsdp")
    ep = lax.axis_index("ep")
    experts, rows, _ = train_gate.shape
    own = experts // n
    band = router.shape[0]

    barrier = pltpu.get_barrier_semaphore()
    for k in range(1, n):
        pl.semaphore_signal(
            barrier, inc=1, device_id={"fsdp": lax.rem(me + k, n)}, device_id_type=MESH
        )
    for k in range(1, groups):
        pl.semaphore_signal(
            barrier, inc=1, device_id={"ep": lax.rem(ep + k, groups)}, device_id_type=MESH
        )

    chips = n // 2
    chip, core = me // 2, lax.rem(me, 2)
    per = 4 * own
    near = jnp.minimum(chip, chips - 1 - chip)
    forward = jnp.where(chip < chips - near - 1, 1, -1)
    both = 2 * near * per
    far = (chips - 1) * per

    def piece_of(t):
        pair = lax.rem(t, 2 * per)
        tail = t - both
        two = t < both
        away = t < far
        shift = jnp.where(
            two,
            (t // (2 * per) + 1) * (1 - 2 * lax.rem(pair, 2)),
            (near + 1 + tail // per) * forward,
        )
        piece = jnp.where(two, pair // 2, lax.rem(tail, per))
        piece = jnp.where(away, piece, t - far)
        to_chip = jnp.where(away, chip + shift, chip)
        which = lax.rem(piece, 2)
        rest = piece // 2
        on_core = jnp.where(away, which, jnp.where(piece < 2 * own, 1 - core, core))
        rest = jnp.where(away, rest, lax.rem(piece, 2 * own))
        return to_chip * 2 + on_core, rest // 2, lax.rem(rest, 2)

    steps = 2 * experts
    remote = steps - 2 * own

    def load(t, act):
        device, expert, tensor = piece_of(t)
        slot = lax.rem(t, SLOTS)
        at = device * own + expert
        for k, (a, b) in enumerate(((train_gate, other_gate), (train_up, other_up))):

            @pl.when(tensor == k)
            def _():
                for source, target, sem in ((a, wide, wide_sem), (b, narrow, narrow_sem)):
                    copy = pltpu.make_async_copy(source.at[at], target.at[slot], sem.at[slot])
                    getattr(copy, act)()

    def ship(t):
        device, expert, tensor = piece_of(t)
        for k, (out, sem) in enumerate(((out_gate, gate_sem), (out_up, up_sem))):
            place = out.at[expert, pl.ds(me * rows, rows), :]

            @pl.when((tensor == k) & (t < remote))
            def _():
                pltpu.make_async_remote_copy(
                    src_ref=send.at[t],
                    dst_ref=place,
                    send_sem=send_sem,
                    recv_sem=sem,
                    device_id={"fsdp": device},
                    device_id_type=MESH,
                ).start()

            @pl.when((tensor == k) & (t >= remote))
            def _():
                pltpu.make_async_copy(send.at[t], place, sem).start()

    for t in range(SLOTS - 1):
        load(t, "start")
    pl.semaphore_wait(barrier, n - 1 + groups - 1)

    home = out_router.at[me, pl.ds(ep * band, band), :]
    pltpu.make_async_copy(router, home, row_recv).start()
    for k in range(1, n):
        pltpu.make_async_remote_copy(
            src_ref=router,
            dst_ref=home,
            send_sem=row_send,
            recv_sem=row_recv,
            device_id={"fsdp": lax.rem(me + k, n)},
            device_id_type=MESH,
        ).start()

    def step(t, _):
        slot = lax.rem(t, SLOTS)

        @pl.when(t + SLOTS - 1 < steps)
        def _():
            load(t + SLOTS - 1, "start")

        load(t, "wait")

        def chunk(r, _):
            at = pl.ds(pl.multiple_of(r * ROWS, ROWS), ROWS)
            latest = wide[slot, at, :] + narrow[slot, at, :].astype(jnp.float32)
            send[t, at, :] = latest.astype(jnp.bfloat16)
            return 0

        lax.fori_loop(0, rows // ROWS, chunk, 0)

        @pl.when(t > 0)
        def _():
            ship(t - 1)

        return 0

    lax.fori_loop(0, steps, step, 0)
    ship(steps - 1)

    columns = out_router.at[:, pl.ds(ep * band, band), :]
    pltpu.make_async_copy(columns, columns, row_recv).wait()
    for k in range(1, groups):
        pltpu.make_async_remote_copy(
            src_ref=columns,
            dst_ref=columns,
            send_sem=col_send,
            recv_sem=col_recv,
            device_id={"ep": lax.rem(ep + k, groups)},
            device_id_type=MESH,
        ).start()
    others = out_router.at[:, pl.ds(0, (groups - 1) * band), :]
    pltpu.make_async_copy(others, others, col_recv).wait()
    pltpu.make_async_copy(others, others, col_send).wait()
    sent = out_router.at[pl.ds(0, n - 1), pl.ds(0, band), :]
    pltpu.make_async_copy(sent, sent, row_send).wait()

    gone = send.at[pl.ds(0, remote)]
    pltpu.make_async_copy(gone, gone, send_sem).wait()
    pltpu.make_async_copy(out_gate, out_gate, gate_sem).wait()
    pltpu.make_async_copy(out_up, out_up, up_sem).wait()


def finish(raw_gate, raw_up, ready_gate, ready_up, scale_gate, scale_up):
    depth, wide = raw_gate.shape[1], raw_gate.shape[2]
    part = 32
    for raw, ready, scale in ((raw_gate, ready_gate, scale_gate), (raw_up, ready_up, scale_up)):

        def add(r, total):
            at = pl.ds(pl.multiple_of(r * part, part), part)
            size = jnp.abs(raw[0, at, :].astype(jnp.float32))
            return total + jnp.sum(size.reshape(part // 8, 8, wide), axis=0)

        total = lax.fori_loop(0, depth // part, add, jnp.zeros((8, wide), jnp.float32))
        mean = jnp.sum(total, axis=0, keepdims=True) / depth
        scale[0] = mean
        over = 1.0 / mean

        def divide(r, _):
            at = pl.ds(pl.multiple_of(r * part, part), part)
            ready[0, at, :] = (raw[0, at, :].astype(jnp.float32) * over).astype(jnp.bfloat16)
            return 0

        lax.fori_loop(0, depth // part, divide, 0)


def shards(n, groups, train_gate, other_gate, train_up, other_up, router_weight, router_gain):
    experts, rows, width = train_gate.shape
    own = experts // n
    part_router = (router_weight * router_gain[:, None]).astype(jnp.bfloat16).T
    band, depth = part_router.shape
    anywhere = pl.BlockSpec(memory_space=pl.ANY)
    landed = jax.ShapeDtypeStruct((own, n * rows, width), jnp.bfloat16)
    raw_gate, raw_up, router = pl.pallas_call(
        functools.partial(exchange, n, groups),
        out_shape=(
            landed,
            landed,
            jax.ShapeDtypeStruct((n, groups * band, depth), jnp.bfloat16),
        ),
        in_specs=[anywhere] * 5,
        out_specs=(anywhere,) * 3,
        scratch_shapes=[
            pltpu.VMEM((SLOTS, rows, width), jnp.float32),
            pltpu.VMEM((SLOTS, rows, width), jnp.bfloat16),
            pltpu.VMEM((2 * experts, rows, width), jnp.bfloat16),
            pltpu.SemaphoreType.DMA((SLOTS,)),
            pltpu.SemaphoreType.DMA((SLOTS,)),
        ]
        + [pltpu.SemaphoreType.DMA] * 7,
        compiler_params=pltpu.CompilerParams(
            collective_id=0, has_side_effects=True, vmem_limit_bytes=56 * 2**20
        ),
    )(train_gate, other_gate, train_up, other_up, part_router)

    cols = 256
    block = pl.BlockSpec((1, n * rows, cols), lambda e, j: (e, 0, j))
    line = pl.BlockSpec((1, 1, cols), lambda e, j: (e, 0, j))
    ready_gate, ready_up, scale_gate, scale_up = pl.pallas_call(
        finish,
        grid=(own, width // cols),
        out_shape=(landed, landed) + (jax.ShapeDtypeStruct((own, 1, width), jnp.float32),) * 2,
        in_specs=[block, block],
        out_specs=(block, block, line, line),
        compiler_params=pltpu.CompilerParams(vmem_limit_bytes=40 * 2**20),
    )(raw_gate, raw_up)
    serve_router = router.transpose(0, 2, 1).reshape(n * depth, groups * band)
    return (
        ready_gate,
        ready_up,
        scale_gate.reshape(own, width),
        scale_up.reshape(own, width),
        serve_router,
    )


def solution(mesh):
    placed = (
        P("ep", "fsdp", None),
        P("ep", "fsdp", None),
        P("ep", "fsdp", None),
        P("ep", "fsdp", None),
        P("fsdp", "ep"),
        P("fsdp"),
    )
    return jax.shard_map(
        functools.partial(shards, mesh.shape["fsdp"], mesh.shape["ep"]),
        mesh=mesh,
        in_specs=placed,
        out_specs=(
            P(("ep", "fsdp"), None, None),
            P(("ep", "fsdp"), None, None),
            P(("ep", "fsdp"), None),
            P(("ep", "fsdp"), None),
            P(),
        ),
        check_vma=False,
    )
```

```python
import functools

import jax
import jax.numpy as jnp
from jax import lax
from jax.experimental import pallas as pl
from jax.experimental.pallas import tpu as pltpu
from jax.sharding import PartitionSpec as P

MESH = pl.DeviceIdType.MESH
SLOTS = 4
ROWS = 32


def exchange(
    n,
    groups,
    train_gate,
    other_gate,
    train_up,
    other_up,
    router,
    mean,
    landed,
    out_router,
    wide,
    narrow,
    send,
    total,
    wide_sem,
    narrow_sem,
    land_sem,
    send_sem,
    row_send,
    row_recv,
    col_send,
    col_recv,
):
    me = lax.axis_index("fsdp")
    ep = lax.axis_index("ep")
    experts, rows, width = train_gate.shape
    own = experts // n
    band = router.shape[0]

    barrier = pltpu.get_barrier_semaphore()
    for k in range(1, n):
        pl.semaphore_signal(
            barrier, inc=1, device_id={"fsdp": lax.rem(me + k, n)}, device_id_type=MESH
        )
    for k in range(1, groups):
        pl.semaphore_signal(
            barrier, inc=1, device_id={"ep": lax.rem(ep + k, groups)}, device_id_type=MESH
        )

    chips = n // 2
    chip, core = me // 2, lax.rem(me, 2)
    per = 4 * own
    near = jnp.minimum(chip, chips - 1 - chip)
    forward = jnp.where(chip < chips - near - 1, 1, -1)
    both = 2 * near * per
    far = (chips - 1) * per

    def piece_of(t):
        pair = lax.rem(t, 2 * per)
        tail = t - both
        two = t < both
        away = t < far
        shift = jnp.where(
            two,
            (t // (2 * per) + 1) * (1 - 2 * lax.rem(pair, 2)),
            (near + 1 + tail // per) * forward,
        )
        piece = jnp.where(two, pair // 2, lax.rem(tail, per))
        piece = jnp.where(away, piece, t - far)
        to_chip = jnp.where(away, chip + shift, chip)
        which = lax.rem(piece, 2)
        rest = piece // 2
        on_core = jnp.where(away, which, jnp.where(piece < 2 * own, 1 - core, core))
        rest = jnp.where(away, rest, lax.rem(piece, 2 * own))
        return to_chip * 2 + on_core, lax.rem(rest, 2), rest // 2

    steps = 2 * experts
    remote = steps - 2 * own

    def load(t, act):
        device, tensor, expert = piece_of(t)
        slot = lax.rem(t, SLOTS)
        at = device * own + expert
        for k, (a, b) in enumerate(((train_gate, other_gate), (train_up, other_up))):

            @pl.when(tensor == k)
            def _():
                for source, target, sem in ((a, wide, wide_sem), (b, narrow, narrow_sem)):
                    copy = pltpu.make_async_copy(source.at[at], target.at[slot], sem.at[slot])
                    getattr(copy, act)()

    def piece_copy(t, source, sem):
        device, tensor, expert = piece_of(t)
        which = tensor * own + expert
        return pltpu.make_async_remote_copy(
            src_ref=send.at[t],
            dst_ref=landed.at[which, pl.ds(source * rows, rows), :],
            send_sem=send_sem,
            recv_sem=land_sem.at[sem, which],
            device_id={"fsdp": device},
            device_id_type=MESH,
        )

    for t in range(SLOTS - 1):
        load(t, "start")
    for k in range(2 * own):
        total[k] = jnp.zeros_like(total[k])
    pl.semaphore_wait(barrier, n - 1 + groups - 1)

    home = out_router.at[me, pl.ds(ep * band, band), :]
    pltpu.make_async_copy(router, home, row_recv).start()
    for k in range(1, n):
        pltpu.make_async_remote_copy(
            src_ref=router,
            dst_ref=home,
            send_sem=row_send,
            recv_sem=row_recv,
            device_id={"fsdp": lax.rem(me + k, n)},
            device_id_type=MESH,
        ).start()

    def fetch(t):
        @pl.when(t + SLOTS - 1 < steps)
        def _():
            load(t + SLOTS - 1, "start")

        load(t, "wait")
        return lax.rem(t, SLOTS)

    def step(t, _):
        slot = fetch(t)

        def chunk(r, _):
            at = pl.ds(pl.multiple_of(r * ROWS, ROWS), ROWS)
            latest = wide[slot, at, :] + narrow[slot, at, :].astype(jnp.float32)
            send[t, at, :] = latest.astype(jnp.bfloat16)
            return 0

        lax.fori_loop(0, rows // ROWS, chunk, 0)

        @pl.when(t > 0)
        def _():
            piece_copy(t - 1, me, me).start()

        return 0

    lax.fori_loop(0, remote, step, 0)
    piece_copy(remote - 1, me, me).start()

    def stay(t, _):
        _, tensor, expert = piece_of(t)
        which = tensor * own + expert
        slot = fetch(t)

        def chunk(r, _):
            at = pl.ds(pl.multiple_of(r * ROWS, ROWS), ROWS)
            to = pl.ds(pl.multiple_of(me * rows + r * ROWS, ROWS), ROWS)
            latest = wide[slot, at, :] + narrow[slot, at, :].astype(jnp.float32)
            landed[which, to, :] = latest.astype(jnp.bfloat16)
            return 0

        lax.fori_loop(0, rows // ROWS, chunk, 0)
        return 0

    lax.fori_loop(remote, steps, stay, 0)

    def fold(which, source):
        def chunk(r, held):
            at = pl.ds(pl.multiple_of(source * rows + r * ROWS, ROWS), ROWS)
            size = jnp.abs(landed[which, at, :].astype(jnp.float32))
            return held + jnp.sum(size.reshape(ROWS // 8, 8, width), axis=0)

        total[which] = lax.fori_loop(0, rows // ROWS, chunk, total[which])

    def fold_own(which, _):
        fold(which, me)
        return 0

    lax.fori_loop(0, 2 * own, fold_own, 0)

    columns = out_router.at[:, pl.ds(ep * band, band), :]
    pltpu.make_async_copy(columns, columns, row_recv).wait()
    for k in range(1, groups):
        pltpu.make_async_remote_copy(
            src_ref=columns,
            dst_ref=columns,
            send_sem=col_send,
            recv_sem=col_recv,
            device_id={"ep": lax.rem(ep + k, groups)},
            device_id_type=MESH,
        ).start()
    others = out_router.at[:, pl.ds(0, (groups - 1) * band), :]
    pltpu.make_async_copy(others, others, col_recv).wait()
    pltpu.make_async_copy(others, others, col_send).wait()
    sent = out_router.at[pl.ds(0, n - 1), pl.ds(0, band), :]
    pltpu.make_async_copy(sent, sent, row_send).wait()

    def take(u, _):
        t = lax.rem(u + far, remote)
        source, tensor, expert = piece_of(t)
        piece_copy(t, source, source).wait_recv()
        fold(tensor * own + expert, source)
        return 0

    lax.fori_loop(0, remote, take, 0)
    for k in range(2 * own):
        mean[pl.ds(k, 1), :] = jnp.sum(total[k], axis=0, keepdims=True) / (n * rows)

    def gone(t, _):
        piece_copy(t, me, me).wait_send()
        return 0

    lax.fori_loop(0, remote, gone, 0)


def finish(own, landed, mean, ready_gate, ready_up, scale_gate, scale_up, held, sem):
    depth = landed.shape[1]
    slots, size, _ = held.shape
    parts = depth // size
    scale_gate[...] = mean[pl.ds(0, own), :]
    scale_up[...] = mean[pl.ds(own, own), :]
    for k in range(2 * own):
        over = 1.0 / mean[pl.ds(k, 1), :]
        out = (ready_gate if k < own else ready_up).at[k % own]

        def put(c, out=out, k=k):
            slot = lax.rem(k * parts + c, slots)
            to = pl.ds(pl.multiple_of(c * size, size), size)
            return pltpu.make_async_copy(held.at[slot], out.at[to, :], sem.at[slot])

        def part(c, _, over=over, put=put, k=k):
            slot = lax.rem(k * parts + c, slots)

            @pl.when(k * parts + c >= slots)
            def _():
                put(c).wait()

            def chunk(r, _):
                at = pl.ds(pl.multiple_of(r * ROWS, ROWS), ROWS)
                of = pl.ds(pl.multiple_of(c * size + r * ROWS, ROWS), ROWS)
                value = landed[k, of, :].astype(jnp.float32) * over
                held[slot, at, :] = value.astype(jnp.bfloat16)
                return 0

            lax.fori_loop(0, size // ROWS, chunk, 0)

            @pl.when(c > 0)
            def _():
                put(c - 1).start()

            return 0

        lax.fori_loop(0, parts, part, 0)
        put(parts - 1).start()
    for slot in range(min(slots, 2 * own * parts)):
        pltpu.make_async_copy(held.at[slot], ready_up.at[0, pl.ds(0, size), :], sem.at[slot]).wait()


def shards(n, groups, train_gate, other_gate, train_up, other_up, router_weight, router_gain):
    experts, rows, width = train_gate.shape
    own = experts // n
    part_router = (router_weight * router_gain[:, None]).astype(jnp.bfloat16).T
    band, depth = part_router.shape
    anywhere = pl.BlockSpec(memory_space=pl.ANY)
    inside = pl.BlockSpec(memory_space=pltpu.VMEM)
    mean, landed, router = pl.pallas_call(
        functools.partial(exchange, n, groups),
        out_shape=(
            pltpu.VMEM((2 * own, width), jnp.float32),
            pltpu.VMEM((2 * own, n * rows, width), jnp.bfloat16),
            jax.ShapeDtypeStruct((n, groups * band, depth), jnp.bfloat16),
        ),
        in_specs=[pl.BlockSpec(memory_space=pltpu.HBM)] * 5,
        out_specs=(inside, inside, anywhere),
        scratch_shapes=[
            pltpu.VMEM((SLOTS, rows, width), jnp.float32),
            pltpu.VMEM((SLOTS, rows, width), jnp.bfloat16),
            pltpu.VMEM((2 * experts - 2 * own, rows, width), jnp.bfloat16),
            pltpu.VMEM((2 * own, 8, width), jnp.float32),
            pltpu.SemaphoreType.DMA((SLOTS,)),
            pltpu.SemaphoreType.DMA((SLOTS,)),
            pltpu.SemaphoreType.DMA((n, 2 * own)),
        ]
        + [pltpu.SemaphoreType.DMA] * 5,
        compiler_params=pltpu.CompilerParams(
            collective_id=0, has_side_effects=True, vmem_limit_bytes=34 * 2**20
        ),
    )(train_gate, other_gate, train_up, other_up, part_router)

    ready = jax.ShapeDtypeStruct((own, n * rows, width), jnp.bfloat16)
    scale = jax.ShapeDtypeStruct((own, width), jnp.float32)
    size = min(256, n * rows)
    ready_gate, ready_up, scale_gate, scale_up = pl.pallas_call(
        functools.partial(finish, own),
        out_shape=(ready, ready, scale, scale),
        in_specs=[inside, inside],
        out_specs=(anywhere, anywhere, inside, inside),
        scratch_shapes=[
            pltpu.VMEM((8, size, width), jnp.bfloat16),
            pltpu.SemaphoreType.DMA((8,)),
        ],
        compiler_params=pltpu.CompilerParams(vmem_limit_bytes=16 * 2**20),
    )(landed, mean)
    serve_router = router.transpose(0, 2, 1).reshape(n * depth, groups * band)
    return ready_gate, ready_up, scale_gate, scale_up, serve_router


def solution(mesh):
    placed = (
        P("ep", "fsdp", None),
        P("ep", "fsdp", None),
        P("ep", "fsdp", None),
        P("ep", "fsdp", None),
        P("fsdp", "ep"),
        P("fsdp"),
    )
    return jax.shard_map(
        functools.partial(shards, mesh.shape["fsdp"], mesh.shape["ep"]),
        mesh=mesh,
        in_specs=placed,
        out_specs=(
            P(("ep", "fsdp"), None, None),
            P(("ep", "fsdp"), None, None),
            P(("ep", "fsdp"), None),
            P(("ep", "fsdp"), None),
            P(),
        ),
        check_vma=False,
    )
```

```python
import functools

import jax
import jax.numpy as jnp
from jax import lax
from jax.experimental import pallas as pl
from jax.experimental.pallas import tpu as pltpu
from jax.sharding import PartitionSpec as P

MESH = pl.DeviceIdType.MESH
SLOTS = 4
ROWS = 32


def exchange(
    n,
    groups,
    train_gate,
    other_gate,
    train_up,
    other_up,
    weight,
    gain,
    mean,
    landed,
    out_router,
    wide,
    narrow,
    send,
    total,
    weight_in,
    gain_in,
    router,
    weight_sem,
    gain_sem,
    wide_sem,
    narrow_sem,
    land_sem,
    send_sem,
    row_send,
    row_recv,
    swap_send,
    swap_recv,
    col_send,
    col_recv,
):
    me = lax.axis_index("fsdp")
    ep = lax.axis_index("ep")
    experts, rows, width = train_gate.shape
    own = experts // n
    band = weight.shape[0]

    barrier = pltpu.get_barrier_semaphore()
    for k in range(1, n):
        pl.semaphore_signal(
            barrier, inc=1, device_id={"fsdp": lax.rem(me + k, n)}, device_id_type=MESH
        )
    for k in range(1, groups):
        pl.semaphore_signal(
            barrier, inc=1, device_id={"ep": lax.rem(ep + k, groups)}, device_id_type=MESH
        )

    chips = n // 2
    chip, core = me // 2, lax.rem(me, 2)
    per = 4 * own
    near = jnp.minimum(chip, chips - 1 - chip)
    forward = jnp.where(chip < chips - near - 1, 1, -1)
    both = 2 * near * per
    far = (chips - 1) * per

    def piece_of(t):
        pair = lax.rem(t, 2 * per)
        tail = t - both
        two = t < both
        away = t < far
        shift = jnp.where(
            two,
            (t // (2 * per) + 1) * (1 - 2 * lax.rem(pair, 2)),
            (near + 1 + tail // per) * forward,
        )
        piece = jnp.where(two, pair // 2, lax.rem(tail, per))
        piece = jnp.where(away, piece, t - far)
        to_chip = jnp.where(away, chip + shift, chip)
        which = lax.rem(piece, 2)
        rest = piece // 2
        on_core = jnp.where(away, which, jnp.where(piece < 2 * own, 1 - core, core))
        rest = jnp.where(away, rest, lax.rem(piece, 2 * own))
        return to_chip * 2 + on_core, lax.rem(rest, 2), rest // 2

    steps = 2 * experts
    remote = steps - 2 * own

    def load(t, act):
        device, tensor, expert = piece_of(t)
        slot = lax.rem(t, SLOTS)
        at = device * own + expert
        for k, (a, b) in enumerate(((train_gate, other_gate), (train_up, other_up))):

            @pl.when(tensor == k)
            def _():
                for source, target, sem in ((a, wide, wide_sem), (b, narrow, narrow_sem)):
                    copy = pltpu.make_async_copy(source.at[at], target.at[slot], sem.at[slot])
                    getattr(copy, act)()

    def piece_copy(t, source, sem):
        device, tensor, expert = piece_of(t)
        which = tensor * own + expert
        return pltpu.make_async_remote_copy(
            src_ref=send.at[t],
            dst_ref=landed.at[which, pl.ds(source * rows, rows), :],
            send_sem=send_sem,
            recv_sem=land_sem.at[sem, which],
            device_id={"fsdp": device},
            device_id_type=MESH,
        )

    for t in range(SLOTS - 1):
        load(t, "start")
    weight_copy = pltpu.make_async_copy(weight, weight_in, weight_sem)
    gain_copy = pltpu.make_async_copy(gain, gain_in, gain_sem)
    weight_copy.start()
    gain_copy.start()
    for k in range(2 * own):
        total[k] = jnp.zeros_like(total[k])
    weight_copy.wait()
    gain_copy.wait()
    router[...] = (weight_in[...] * gain_in[...]).astype(jnp.bfloat16)
    pl.semaphore_wait(barrier, n - 1 + groups - 1)

    home = out_router.at[chip, core, pl.ds(ep * band, band), :]
    pltpu.make_async_copy(router, home, row_recv).start()
    for k in range(1, chips):
        pltpu.make_async_remote_copy(
            src_ref=router,
            dst_ref=home,
            send_sem=row_send,
            recv_sem=row_recv,
            device_id={"fsdp": lax.rem(chip + k, chips) * 2 + core},
            device_id_type=MESH,
        ).start()

    def fetch(t):
        @pl.when(t + SLOTS - 1 < steps)
        def _():
            load(t + SLOTS - 1, "start")

        load(t, "wait")
        return lax.rem(t, SLOTS)

    def step(t, _):
        slot = fetch(t)

        def chunk(r, _):
            at = pl.ds(pl.multiple_of(r * ROWS, ROWS), ROWS)
            latest = wide[slot, at, :] + narrow[slot, at, :].astype(jnp.float32)
            send[t, at, :] = latest.astype(jnp.bfloat16)
            return 0

        lax.fori_loop(0, rows // ROWS, chunk, 0)

        @pl.when(t > 0)
        def _():
            piece_copy(t - 1, me, me).start()

        return 0

    lax.fori_loop(0, remote, step, 0)
    piece_copy(remote - 1, me, me).start()

    def stay(t, _):
        _, tensor, expert = piece_of(t)
        which = tensor * own + expert
        slot = fetch(t)

        def chunk(r, _):
            at = pl.ds(pl.multiple_of(r * ROWS, ROWS), ROWS)
            to = pl.ds(pl.multiple_of(me * rows + r * ROWS, ROWS), ROWS)
            latest = wide[slot, at, :] + narrow[slot, at, :].astype(jnp.float32)
            landed[which, to, :] = latest.astype(jnp.bfloat16)
            return 0

        lax.fori_loop(0, rows // ROWS, chunk, 0)
        return 0

    lax.fori_loop(remote, steps, stay, 0)

    def fold(which, source):
        def chunk(r, held):
            at = pl.ds(pl.multiple_of(source * rows + r * ROWS, ROWS), ROWS)
            size = jnp.abs(landed[which, at, :].astype(jnp.float32))
            return held + jnp.sum(size.reshape(ROWS // 8, 8, width), axis=0)

        total[which] = lax.fori_loop(0, rows // ROWS, chunk, total[which])

    def fold_own(which, _):
        fold(which, me)
        return 0

    lax.fori_loop(0, 2 * own, fold_own, 0)

    mine = out_router.at[:, core, pl.ds(ep * band, band), :]
    pltpu.make_async_copy(mine, mine, row_recv).wait()
    swap = pltpu.make_async_remote_copy(
        src_ref=mine,
        dst_ref=mine,
        send_sem=swap_send,
        recv_sem=swap_recv,
        device_id={"fsdp": chip * 2 + 1 - core},
        device_id_type=MESH,
    )
    swap.start()
    swap.wait()
    columns = out_router.at[:, :, pl.ds(ep * band, band), :]
    for k in range(1, groups):
        pltpu.make_async_remote_copy(
            src_ref=columns,
            dst_ref=columns,
            send_sem=col_send,
            recv_sem=col_recv,
            device_id={"ep": lax.rem(ep + k, groups)},
            device_id_type=MESH,
        ).start()
    others = out_router.at[:, :, pl.ds(0, (groups - 1) * band), :]
    pltpu.make_async_copy(others, others, col_recv).wait()
    pltpu.make_async_copy(others, others, col_send).wait()
    sent = out_router.at[pl.ds(0, chips - 1), 0, pl.ds(0, band), :]
    pltpu.make_async_copy(sent, sent, row_send).wait()

    def take(u, _):
        t = lax.rem(u + far, remote)
        source, tensor, expert = piece_of(t)
        piece_copy(t, source, source).wait_recv()
        fold(tensor * own + expert, source)
        return 0

    lax.fori_loop(0, remote, take, 0)
    for k in range(2 * own):
        mean[pl.ds(k, 1), :] = jnp.sum(total[k], axis=0, keepdims=True) / (n * rows)

    pltpu.make_async_copy(send, send, send_sem).wait()


def finish(
    own,
    landed,
    mean,
    ready_gate,
    ready_up,
    scale_gate,
    scale_up,
    held,
    sem,
):
    depth = landed.shape[1]
    slots, size, _ = held.shape
    parts = depth // size
    scale_gate[...] = mean[pl.ds(0, own), :]
    scale_up[...] = mean[pl.ds(own, own), :]
    for k in range(2 * own):
        over = 1.0 / mean[pl.ds(k, 1), :]
        out = (ready_gate if k < own else ready_up).at[k % own]

        def put(c, out=out, k=k):
            slot = lax.rem(k * parts + c, slots)
            to = pl.ds(pl.multiple_of(c * size, size), size)
            return pltpu.make_async_copy(held.at[slot], out.at[to, :], sem.at[slot])

        def part(c, _, over=over, put=put, k=k):
            slot = lax.rem(k * parts + c, slots)

            @pl.when(k * parts + c >= slots)
            def _():
                put(c).wait()

            def chunk(r, _):
                at = pl.ds(pl.multiple_of(r * ROWS, ROWS), ROWS)
                of = pl.ds(pl.multiple_of(c * size + r * ROWS, ROWS), ROWS)
                value = landed[k, of, :].astype(jnp.float32) * over
                held[slot, at, :] = value.astype(jnp.bfloat16)
                return 0

            lax.fori_loop(0, size // ROWS, chunk, 0)

            @pl.when(c > 0)
            def _():
                put(c - 1).start()

            return 0

        lax.fori_loop(0, parts, part, 0)
        put(parts - 1).start()
    for slot in range(min(slots, 2 * own * parts)):
        pltpu.make_async_copy(held.at[slot], ready_up.at[0, pl.ds(0, size), :], sem.at[slot]).wait()


def shards(n, groups, train_gate, other_gate, train_up, other_up, router_weight, router_gain):
    experts, rows, width = train_gate.shape
    own = experts // n
    depth, band = router_weight.shape
    anywhere = pl.BlockSpec(memory_space=pl.ANY)
    outside = pl.BlockSpec(memory_space=pltpu.HBM)
    inside = pl.BlockSpec(memory_space=pltpu.VMEM)
    mean, landed, router = pl.pallas_call(
        functools.partial(exchange, n, groups),
        out_shape=(
            pltpu.VMEM((2 * own, width), jnp.float32),
            pltpu.VMEM((2 * own, n * rows, width), jnp.bfloat16),
            pltpu.HBM((n // 2, 2, groups * band, depth), jnp.bfloat16),
        ),
        in_specs=[outside] * 6,
        out_specs=(inside, inside, outside),
        scratch_shapes=[
            pltpu.VMEM((SLOTS, rows, width), jnp.float32),
            pltpu.VMEM((SLOTS, rows, width), jnp.bfloat16),
            pltpu.VMEM((2 * experts - 2 * own, rows, width), jnp.bfloat16),
            pltpu.VMEM((2 * own, 8, width), jnp.float32),
            pltpu.VMEM((band, depth), jnp.float32),
            pltpu.VMEM((1, depth), jnp.float32),
            pltpu.VMEM((band, depth), jnp.bfloat16),
            pltpu.SemaphoreType.DMA,
            pltpu.SemaphoreType.DMA,
            pltpu.SemaphoreType.DMA((SLOTS,)),
            pltpu.SemaphoreType.DMA((SLOTS,)),
            pltpu.SemaphoreType.DMA((n, 2 * own)),
        ]
        + [pltpu.SemaphoreType.DMA] * 7,
        compiler_params=pltpu.CompilerParams(
            collective_id=0, has_side_effects=True, vmem_limit_bytes=34 * 2**20
        ),
    )(train_gate, other_gate, train_up, other_up, router_weight.T, router_gain[None])

    ready = jax.ShapeDtypeStruct((own, n * rows, width), jnp.bfloat16)
    scale = jax.ShapeDtypeStruct((own, width), jnp.float32)
    size = min(256, n * rows)
    ready_gate, ready_up, scale_gate, scale_up = pl.pallas_call(
        functools.partial(finish, own),
        out_shape=(
            ready,
            ready,
            scale,
            scale,
        ),
        in_specs=[inside, inside],
        out_specs=(anywhere, anywhere, inside, inside),
        scratch_shapes=[
            pltpu.VMEM((8, size, width), jnp.bfloat16),
            pltpu.SemaphoreType.DMA((8,)),
        ],
        compiler_params=pltpu.CompilerParams(vmem_limit_bytes=16 * 2**20),
    )(landed, mean)
    serve_router = router.transpose(0, 1, 3, 2).reshape(n * depth, groups * band)
    return ready_gate, ready_up, scale_gate, scale_up, serve_router


def solution(mesh):
    placed = (
        P("ep", "fsdp", None),
        P("ep", "fsdp", None),
        P("ep", "fsdp", None),
        P("ep", "fsdp", None),
        P("fsdp", "ep"),
        P("fsdp"),
    )
    return jax.shard_map(
        functools.partial(shards, mesh.shape["fsdp"], mesh.shape["ep"]),
        mesh=mesh,
        in_specs=placed,
        out_specs=(
            P(("ep", "fsdp"), None, None),
            P(("ep", "fsdp"), None, None),
            P(("ep", "fsdp"), None),
            P(("ep", "fsdp"), None),
            P(),
        ),
        check_vma=False,
    )
```
